32 devices in a mesh: seq: 4 (over z), bal: 4 (over y, x), rep: 2 (over core).
Axes of the slice: x: 2, y: 2, z: 4, core: 2. Of those that a mesh axis runs over, the one named last changes fastest.
Arguments:
- queries: bfloat16 [8, 6, 512, 2048], P('rep', None, ('seq', 'bal')), parts along dimension 0, may hold values from -16 to 16
- key_tokens: bfloat16 [8, 6, 512, 2048], P('rep', None, ('seq', 'bal')), parts along dimension 0, may hold values from -8 to 8
- value_tokens: bfloat16 [8, 6, 512, 2048], P('rep', None, ('seq', 'bal')), parts along dimension 0, may hold values from -6 to 6
- view_lists: int32 [8, 6, 4], P('rep'), parts along dimension 0, may hold values from -1 to 5, as said below
Outputs:
- attended: bfloat16 [8, 6, 512, 2048], P('rep', None, ('seq', 'bal')), parts along dimension 0
The draws below stay inside these ranges and needn't reach their ends.
There are 2 independent parts, one for each index of `rep`. The reference program is written for one: setup_inputs(seed, part) draws one part's arguments, and reference() takes and returns one part's arrays. A program takes and returns all parts, laid end to end along the dimension named above; each array names one. Nothing has to cross between parts.
Inputs may be any that keep to these rules, and one draw needn't show every extreme that they name: Each list view_lists[w, v] begins with v itself, names distinct views, and holds -1 in every entry after its named views; in every draw some list names 4 views.
All inputs are finite; a program needn't handle non-finite values.
Results may differ from the reference program's by a relative error of at most 0.003.
Values may be sent and summed in bfloat16 or wider, within the bound.
No kernel may reach another device: no remote copies, remote signals or barrier semaphores. Data moves between devices by JAX's collectives and lax.ppermute only.
A program may use at most 64 MiB of HBM per device.

```python
import math
import jax
import jax.numpy as jnp
from jax import lax

HEAD = 128
D = 2048
VIEWS = 6
KMAX = 4
WTOK = 512
WINDOWS = 4


def draw_queries(key, part):
    shape = (WINDOWS, VIEWS, WTOK, D)
    scale_shape = (WINDOWS, VIEWS, WTOK, 1)
    base_noise = jnp.clip(jax.random.normal(jax.random.fold_in(key, 11), shape, jnp.float32), -4.0, 4.0)
    row_scale = jnp.exp(jax.random.uniform(jax.random.fold_in(key, 12), scale_shape, jnp.float32, math.log(0.4), math.log(4.0)))
    values = base_noise * row_scale
    return values.astype(jnp.bfloat16)


def draw_key_tokens(key, part):
    shape = (WINDOWS, VIEWS, WTOK, D)
    scale_shape = (WINDOWS, VIEWS, WTOK, 1)
    base_noise = jnp.clip(jax.random.normal(jax.random.fold_in(key, 21), shape, jnp.float32), -4.0, 4.0)
    row_scale = jnp.exp(jax.random.uniform(jax.random.fold_in(key, 22), scale_shape, jnp.float32, math.log(0.5), math.log(2.0)))
    values = base_noise * row_scale
    return values.astype(jnp.bfloat16)


def one_order(sub_key):
    return jax.random.permutation(sub_key, VIEWS)


def draw_view_lists(key, part):
    dense_window = jax.random.randint(jax.random.fold_in(key, 5), (), 0, WINDOWS)
    grid_keys = jax.random.split(jax.random.fold_in(key, 6), WINDOWS * VIEWS)
    orders = jax.vmap(one_order)(grid_keys).reshape(WINDOWS, VIEWS, VIEWS).astype(jnp.int32)
    self_ids = jnp.arange(VIEWS, dtype=jnp.int32)[None, :, None]
    position = jnp.arange(VIEWS, dtype=jnp.int32)[None, None, :]
    ranking = jnp.where(orders == self_ids, -1, position)
    placement = jnp.argsort(ranking, axis=-1, stable=True)
    listed = jnp.take_along_axis(orders, placement, axis=-1)[:, :, :KMAX]
    extra = (jax.random.randint(jax.random.fold_in(key, 7), (WINDOWS, VIEWS), 0, 4) == 0).astype(jnp.int32)
    window_ids = jnp.arange(WINDOWS, dtype=jnp.int32)[:, None]
    lengths = jnp.where(window_ids == dense_window, KMAX, 1 + extra)
    slot_ids = jnp.arange(KMAX, dtype=jnp.int32)[None, None, :]
    return jnp.where(slot_ids < lengths[:, :, None], listed, -1).astype(jnp.int32)


def block_scale(stream_key, shape, cuts, smallest, high):
    def one(dim, parts):
        draws = jax.random.uniform(jax.random.fold_in(jax.random.fold_in(stream_key, 6), dim), (parts,), jnp.float32, smallest / len(cuts), high / len(cuts))
        return jnp.repeat(jnp.exp(draws), shape[dim] // parts).reshape((-1,) + (1,) * (len(shape) - dim - 1))

    level = one(*cuts[0])
    for cut in cuts[1:]:
        level = level * one(*cut)
    return level


def bell_draw(rng, dims, spread, reach, shards=(), kind=jnp.bfloat16):
    values = spread * jax.random.normal(rng, dims, jnp.float32)
    if shards:
        values = values * block_scale(rng, dims, shards, -0.22, 0.18)
    return jnp.clip(values, -reach, reach).astype(kind)


def setup_inputs(seed: int = 0, part: int = 0) -> dict:
    key_of = jax.random.split(jax.random.key(seed), 5)
    part_splits = jax.random.split(jax.random.fold_in(key_of[4], part), 5)
    return {
        "queries": draw_queries(jax.random.fold_in(jax.random.fold_in(key_of[4], part), 71), part),
        "key_tokens": draw_key_tokens(jax.random.fold_in(jax.random.fold_in(key_of[4], part), 71), part),
        "value_tokens": bell_draw(part_splits[2], (WINDOWS, VIEWS, WTOK, D), 1.0, 6.0, ((2, 16),)),
        "view_lists": draw_view_lists(jax.random.fold_in(jax.random.fold_in(key_of[4], part), 71), part),
    }


def reference(queries, key_tokens, value_tokens, view_lists):
    windows, view_count, row_count, feature_width = queries.shape
    head_count = feature_width // HEAD
    score_scale = 1.0 / math.sqrt(HEAD)
    view_ids = jnp.arange(view_count, dtype=jnp.int32)
    outputs = []
    for window in range(windows):
        key_all = key_tokens[window].astype(jnp.float32).reshape(view_count * row_count, head_count, HEAD)
        value_all = value_tokens[window].astype(jnp.float32).reshape(view_count * row_count, head_count, HEAD)
        per_view = []
        for view in range(view_count):
            view_row = view_lists[window, view]
            allowed = jnp.any(view_row[:, None] == view_ids[None, :], axis=0)
            key_mask = jnp.repeat(allowed, row_count)
            query_rows = queries[window, view].astype(jnp.float32).reshape(row_count, head_count, HEAD)
            scores = jnp.einsum('qhd,khd->hqk', query_rows, key_all) * score_scale
            scores = jnp.where(key_mask[None, None, :], scores, -jnp.inf)
            row_top = lax.optimization_barrier(jnp.max(scores, axis=2))
            exponent = jnp.exp(scores - row_top[:, :, None])
            row_total = lax.optimization_barrier(jnp.sum(exponent, axis=2))
            weights = lax.optimization_barrier(exponent.astype(jnp.bfloat16))
            mixed = jnp.einsum('hqk,khd->qhd', weights.astype(jnp.float32), value_all)
            mixed = mixed / jnp.transpose(row_total)[:, :, None]
            per_view.append(mixed.reshape(row_count, feature_width).astype(jnp.bfloat16))
        outputs.append(jnp.stack(per_view))
    return jnp.stack(outputs)
```

```python
import math

import jax
import jax.numpy as jnp
from jax import lax
from jax.experimental import pallas as pl
from jax.experimental.pallas import tpu as pltpu
from jax.sharding import PartitionSpec as P

HEAD = 128
AXES = ("seq", "bal")


class Plan:
    def __init__(self, shape, group):
        self.windows, self.views, self.rows, width = shape
        heads = width // HEAD
        self.group = group
        self.head_parts = math.gcd(heads, group)
        self.window_parts = group // self.head_parts
        self.local_heads = heads // self.head_parts
        self.columns = self.local_heads * HEAD
        self.chunks = self.windows // self.window_parts
        self.paired = group & (group - 1) == 0
        self.tokens = group * self.rows

    def partner(self, me, hop):
        if self.paired:
            return jnp.bitwise_xor(me, hop)
        return lax.rem(me + hop, self.group)

    def source(self, me, hop):
        if self.paired:
            return jnp.bitwise_xor(me, hop)
        return lax.rem(me + self.group - hop, self.group)

    def permutation(self, hop):
        if self.paired:
            return [(i, i ^ hop) for i in range(self.group)]
        return [(i, (i + hop) % self.group) for i in range(self.group)]

    def place(self, device):
        column = lax.rem(device, self.head_parts) * self.columns
        return lax.div(device, self.head_parts), pl.multiple_of(column, HEAD)


def whole():
    return pl.BlockSpec(memory_space=pltpu.VMEM)


def attend(plan, me, lists, held, result, top, total, mixed):
    factor = math.log2(math.e) / math.sqrt(HEAD)
    tile = min(256, plan.tokens)
    blocks = tile // plan.rows
    window = lax.div(me, plan.head_parts)

    def tile_of(part, view, start, h):
        picked = held[part, view, pl.ds(start, blocks), :, h * HEAD : (h + 1) * HEAD]
        return picked.reshape(tile, HEAD)

    def all_of(part, view, h):
        picked = held[part, view, :, :, h * HEAD : (h + 1) * HEAD]
        return picked.reshape(plan.tokens, HEAD)

    def scores(view, key_view, i, h):
        return lax.dot_general(
            tile_of(0, view, i * blocks, h),
            all_of(1, key_view, h),
            (((1,), (1,)), ((), ())),
            preferred_element_type=jnp.float32,
        )

    def weigh(exponent, key_view, h):
        return jnp.dot(
            exponent.astype(jnp.bfloat16),
            all_of(2, key_view, h),
            preferred_element_type=jnp.float32,
        )

    def per_view(view, _):
        for h in range(plan.local_heads):
            for i in range(plan.tokens // tile):
                rows = pl.ds(i * tile, tile)
                s = scores(view, view, i, h)
                new_top = jnp.max(s, axis=1, keepdims=True)
                exponent = jnp.exp2(s * factor - new_top * factor)
                top[h, rows] = new_top
                total[h, rows] = jnp.sum(exponent, axis=1, keepdims=True)
                mixed[h, rows] = weigh(exponent, view, h)

        def more(slot, _):
            key_view = lists[window, view, slot]

            @pl.when(key_view >= 0)
            def _():
                for h in range(plan.local_heads):
                    for i in range(plan.tokens // tile):
                        rows = pl.ds(i * tile, tile)
                        s = scores(view, key_view, i, h)
                        old_top = top[h, rows]
                        new_top = jnp.maximum(old_top, jnp.max(s, axis=1, keepdims=True))
                        rescale = jnp.exp2((old_top - new_top) * factor)
                        exponent = jnp.exp2(s * factor - new_top * factor)
                        top[h, rows] = new_top
                        total[h, rows] = total[h, rows] * rescale + jnp.sum(
                            exponent, axis=1, keepdims=True
                        )
                        mixed[h, rows] = mixed[h, rows] * rescale + weigh(
                            exponent, key_view, h
                        )

            return 0

        lax.fori_loop(1, lists.shape[2], more, 0)
        for h in range(plan.local_heads):
            done = (mixed[h] / total[h]).astype(jnp.bfloat16)
            result[view, :, :, h * HEAD : (h + 1) * HEAD] = done.reshape(
                plan.group, plan.rows, HEAD
            )
        return 0

    lax.fori_loop(0, plan.views, per_view, 0)


def step_kernel(plan, attends, packs, *refs):
    refs = list(refs)
    me = refs.pop(0)[0]
    if attends:
        lists = refs.pop(0)
        arrived = [refs.pop(0) for _ in range(plan.group)]
    tokens = [refs.pop(0) for _ in range(3)] if packs else []
    pieces = [refs.pop(0) for _ in range(plan.group)]
    if packs:
        for hop in range(plan.group):
            window, column = plan.place(plan.partner(me, hop))
            for part in range(3):
                pieces[hop][part] = tokens[part][window, :, :, pl.ds(column, plan.columns)]
    if attends:
        held, result, top, total, mixed = refs
        for hop in range(plan.group):
            source = plan.source(me, hop)
            for part in range(3):
                held[part, :, source] = arrived[hop][part]
        attend(plan, me, lists, held, result, top, total, mixed)
        for hop in range(plan.group):
            pieces[hop][3 if packs else 0] = result[:, plan.partner(me, hop)]


def step(plan, chunk, me, lists, arrived, tokens):
    attends, packs = arrived is not None, tokens is not None
    parts = (3 if packs else 0) + (1 if attends else 0)
    args, specs, scratch = [me], [pl.BlockSpec(memory_space=pltpu.SMEM)], []
    flops = 0
    if attends:
        args += [lists, *arrived]
        specs += [pl.BlockSpec(memory_space=pltpu.SMEM)] + [whole()] * plan.group
        held = (plan.views, plan.group, plan.rows, plan.columns)
        state = (plan.local_heads, plan.tokens)
        scratch = [
            pltpu.VMEM((3, *held), jnp.bfloat16),
            pltpu.VMEM(held, jnp.bfloat16),
            pltpu.VMEM((*state, 1), jnp.float32),
            pltpu.VMEM((*state, 1), jnp.float32),
            pltpu.VMEM((*state, HEAD), jnp.float32),
        ]
        flops = 8 * plan.views * plan.tokens * plan.tokens * plan.columns
    if packs:
        args += tokens
        block = (plan.window_parts, *tokens[0].shape[1:])
        specs += [pl.BlockSpec(block, lambda i: (chunk, 0, 0, 0))] * 3
    piece = (parts, plan.views, plan.rows, plan.columns)
    return pl.pallas_call(
        lambda *refs: step_kernel(plan, attends, packs, *refs),
        grid=(1,),
        out_shape=[jax.ShapeDtypeStruct(piece, jnp.bfloat16)] * plan.group,
        in_specs=specs,
        out_specs=[whole()] * plan.group,
        scratch_shapes=scratch,
        name=f"step_a{int(attends)}p{int(packs)}",
        cost_estimate=pl.CostEstimate(
            flops=flops, bytes_accessed=2 * plan.group * math.prod(piece) * 2, transcendentals=0
        ),
    )(*args)


def unpack_kernel(plan, *refs):
    me = refs[0][0]
    out = refs[-1]
    for hop in range(plan.group):
        piece = refs[1 + hop]
        window, column = plan.place(plan.source(me, hop))
        out[window, :, :, pl.ds(column, plan.columns)] = piece[0]


def unpack(plan, chunk, me, arrived, shape, before):
    last = arrived[0].shape[0] - 1
    piece = pl.BlockSpec((1, *arrived[0].shape[1:]), lambda i: (last, 0, 0, 0))
    args = [me, *arrived]
    specs = [pl.BlockSpec(memory_space=pltpu.SMEM)] + [piece] * plan.group
    aliases = {}
    if before is not None:
        aliases = {len(args): 0}
        args.append(before)
        specs.append(pl.BlockSpec(memory_space=pl.ANY))
    return pl.pallas_call(
        lambda *refs: unpack_kernel(plan, *refs),
        grid=(1,),
        out_shape=jax.ShapeDtypeStruct(shape, jnp.bfloat16),
        in_specs=specs,
        out_specs=pl.BlockSpec((plan.window_parts, *shape[1:]), lambda i: (chunk, 0, 0, 0)),
        input_output_aliases=aliases,
        name="unpack",
        cost_estimate=pl.CostEstimate(flops=0, bytes_accessed=1 << 20, transcendentals=0),
    )(*args)


def local(queries, key_tokens, value_tokens, view_lists):
    plan = Plan(queries.shape, lax.axis_size(AXES))
    me = lax.axis_index(AXES).astype(jnp.int32)
    me_array = jnp.full((1,), me, jnp.int32)
    hops = sorted(range(1, plan.group), reverse=True)
    steps = plan.chunks + 2
    received = []
    out = None
    for i in range(steps):
        tokens = (queries, key_tokens, value_tokens) if i < plan.chunks else None
        arrived, lists = None, None
        if i >= 2:
            arrived = received[i - 2]
            lists = lax.dynamic_slice_in_dim(
                view_lists, (i - 2) * plan.window_parts, plan.window_parts, 0
            )
        pieces = step(plan, i, me_array, lists, arrived, tokens)
        landed = [pieces[0]] + [None] * (plan.group - 1)
        for hop in hops:
            landed[hop] = lax.ppermute(pieces[hop], AXES, plan.permutation(hop))
        received.append(landed)
    for chunk in range(plan.chunks):
        out = unpack(plan, chunk, me_array, received[chunk + 2], queries.shape, out)
    return out


def solution(mesh):
    return jax.shard_map(
        local,
        mesh=mesh,
        in_specs=(
            P("rep", None, AXES, None),
            P("rep", None, AXES, None),
            P("rep", None, AXES, None),
            P("rep", None, None),
        ),
        out_specs=P("rep", None, AXES, None),
        check_vma=False,
    )
```
